32 devices in a mesh: node: 32 (over z, y, x, core).
Axes of the slice: x: 2, y: 2, z: 4, core: 2. Of those that a mesh axis runs over, the one named last changes fastest.
Arguments:
- params: float32 [16384, 2048], P('node'), may hold values from -6 to 6
- public: float32 [16384, 2048], P('node'), may hold values from -4 to 4
- peer_public: float32 [16384, 2048], P('node'), may hold values from -8 to 8
- round_index: int32 [1], replicated, may hold values from 0 to 63
Outputs:
- params_new: float32 [16384, 2048], P('node')
- public_new: float32 [16384, 2048], P('node')
- peer_public_new: float32 [16384, 2048], P('node')
- consensus_gap: float32 [], replicated
The draws below stay inside these ranges and needn't reach their ends.
All inputs are finite; a program needn't handle non-finite values.
Results may differ from the reference program's by a relative error of at most 0.0003.
Values may be sent and summed in bfloat16 or wider, within the bound.
A program may use at most 128 MiB of HBM per device.

```python
import jax
import jax.numpy as jnp

D = 2048
ROWS = 512
BLOCK = 128
NODES = 32
N_NODE = 32


def lattice_pair(key):
    base_key = jax.random.fold_in(key, 7)
    keys = jax.random.split(base_key, 8)
    block_count = NODES * ROWS // BLOCK
    shape = (block_count, BLOCK, D)
    worker_factor = jax.random.uniform(keys[7], (NODES,), jnp.float32, 0.1, 1.0)
    block_worker = jnp.arange(block_count, dtype=jnp.int32) // (ROWS // BLOCK)
    block_factor = jnp.take(worker_factor, block_worker, axis=0)[:, None, None]
    public = jnp.clip(jax.random.normal(keys[0], shape, jnp.float32), -4.0, 4.0)
    scale = jnp.exp(jax.random.uniform(keys[1], (block_count, 1, D), jnp.float32, jnp.log(0.1), jnp.log(1.0)))
    offset = jax.random.uniform(keys[2], shape, jnp.float32, 0.1, 0.4)
    public = public * block_factor
    scale = scale.astype(jnp.bfloat16).astype(jnp.float32)
    level = jax.random.randint(keys[3], shape, -126, 127).astype(jnp.float32)
    sign_bits = jax.random.randint(keys[4], shape, 0, 2)
    signed_offset = jnp.where(sign_bits == 1, offset, -offset)
    value = level + signed_offset
    value = jnp.clip(value, -126.45, 126.45)
    pick = jax.random.randint(keys[5], (block_count, 1, D), 0, BLOCK)
    rows = jnp.arange(BLOCK, dtype=jnp.int32)[None, :, None]
    peak_sign = jnp.where(jax.random.randint(keys[6], (block_count, 1, D), 0, 2) == 1, 1.0, -1.0)
    delta = scale * value / 127.0
    delta = jnp.where(rows == pick, peak_sign * scale, delta)
    params = public + delta
    return (params.reshape(NODES * ROWS, D), public.reshape(NODES * ROWS, D))


def draw_params(key, part):
    return lattice_pair(key)[0]


def draw_public(key, part):
    return lattice_pair(key)[1]


def draw_peer_public(key, part):
    keys = jax.random.split(jax.random.fold_in(key, 11), 4)
    worker_ids = jnp.arange(NODES * ROWS, dtype=jnp.int32) // ROWS
    ramp_all = jnp.arange(NODES, dtype=jnp.float32) / jnp.float32(max(NODES - 1, 1))
    ramp_low = jax.random.uniform(keys[1], (), jnp.float32, 0.25, 0.5)
    ramp_high = jax.random.uniform(keys[2], (), jnp.float32, 1.0, 1.6)
    jitter = jnp.exp(jax.random.uniform(keys[3], (NODES,), jnp.float32, jnp.log(0.7), jnp.log(1.25)))
    base = jnp.clip(jax.random.normal(keys[0], (NODES * ROWS, D), jnp.float32), -4.0, 4.0)
    worker_factor = (ramp_low + (ramp_high - ramp_low) * ramp_all) * jitter
    row_factor = jnp.take(worker_factor, worker_ids, axis=0)
    return base * row_factor[:, None]


def setup_inputs(seed: int = 0) -> dict:
    splits = jax.random.split(jax.random.key(seed), 5)
    return {
        "params": draw_params(jax.random.fold_in(splits[4], 71), 0),
        "public": draw_public(jax.random.fold_in(splits[4], 71), 0),
        "peer_public": draw_peer_public(jax.random.fold_in(splits[4], 71), 0),
        "round_index": jax.random.randint(splits[3], (1,), 0, 64).astype(jnp.int32),
    }


def reference(params, public, peer_public, round_index):
    bit_count = N_NODE.bit_length() - 1
    chosen_bit = round_index[0] % bit_count
    offset = jnp.left_shift(jnp.int32(1), chosen_bit.astype(jnp.int32))
    node_ids = jnp.arange(NODES, dtype=jnp.int32)
    partner = jnp.bitwise_xor(node_ids, offset).astype(jnp.int32)
    difference = (params - public).reshape(NODES, ROWS // BLOCK, BLOCK, D)
    block_peak = jnp.max(jnp.abs(difference), axis=2) + 1e-6
    block_scale = block_peak.astype(jnp.bfloat16)
    wide_scale = block_scale.astype(jnp.float32)[:, :, None, :]
    coded = jnp.floor((difference / wide_scale) * 127.0 + 0.5).astype(jnp.bfloat16)
    own_delta = (coded.astype(jnp.float32) * wide_scale) / 127.0
    partner_delta = jnp.take(own_delta, partner, axis=0)
    own_delta = own_delta.reshape(NODES * ROWS, D)
    partner_delta = partner_delta.reshape(NODES * ROWS, D)
    public_new = public + own_delta
    peer_public_new = peer_public + partner_delta
    params_new = params + 0.4 * (peer_public_new - public_new)
    distance = params_new - public_new
    consensus_gap = jnp.sum(distance * distance) / jnp.float32(NODES * ROWS * D)
    return params_new, public_new, peer_public_new, consensus_gap
```

```python
from functools import partial

import jax
import jax.numpy as jnp
from jax import lax
from jax.experimental import pallas as pl
from jax.experimental.pallas import tpu as pltpu
from jax.sharding import PartitionSpec as P

BLOCK = 128
MIX = 0.4


def chunk_list(row_count, col_count):
    blocks = row_count // BLOCK
    small = col_count // 4
    pieces = []
    for b in range(blocks):
        if b == 0:
            pieces += [(b, 0, 2 * small), (b, 2 * small, col_count - 2 * small)]
        elif b == blocks - 1:
            pieces += [(b, 0, col_count - small), (b, col_count - small, small)]
        else:
            pieces += [(b, 0, col_count)]
    return pieces


def enc_kernel(*refs):
    params_ref, public_ref = refs[:2]
    coded_ref, scale_ref, public_new_ref = refs[-3:]
    public = public_ref[...]
    difference = params_ref[...] - public
    peak = jnp.max(jnp.abs(difference), axis=0, keepdims=True) + 1e-06
    scale = peak.astype(jnp.bfloat16)
    wide = scale.astype(jnp.float32)
    level = jnp.floor(difference / wide * 127.0 + 0.5)
    coded_ref[...] = level.astype(jnp.bfloat16)
    scale_ref[...] = scale
    public_new_ref[...] = public + level * wide * (1.0 / 127.0)


def cost(count, reads, writes):
    return pl.CostEstimate(flops=12 * count, bytes_accessed=count * (reads + writes), transcendentals=0)


def encode(params, public, public_new, piece):
    b, c0, cw = piece
    tile = min(256, cw)
    base = c0 // tile
    here = pl.BlockSpec((BLOCK, tile), lambda j: (b, base + j))
    any_spec = pl.BlockSpec(memory_space=pl.ANY)
    args, specs, aliases = [params, public], [here, here], {}
    if public_new is not None:
        args.append(public_new)
        specs.append(any_spec)
        aliases = {2: 2}
    return pl.pallas_call(
        enc_kernel,
        grid=(cw // tile,),
        in_specs=specs,
        out_specs=[
            pl.BlockSpec((BLOCK, tile), lambda j: (0, j)),
            pl.BlockSpec((1, tile), lambda j: (0, j)),
            here,
        ],
        out_shape=[
            jax.ShapeDtypeStruct((BLOCK, cw), jnp.bfloat16),
            jax.ShapeDtypeStruct((1, cw), jnp.bfloat16),
            jax.ShapeDtypeStruct(params.shape, jnp.float32),
        ],
        input_output_aliases=aliases,
        cost_estimate=cost(BLOCK * cw, 8, 6),
        compiler_params=pltpu.CompilerParams(vmem_limit_bytes=8 << 20),
    )(*args)


def comb_kernel(params_ref, public_new_ref, peer_ref, coded_ref, scale_ref, acc_ref, *refs):
    params_out, peer_out, acc_out = refs[-3:]

    @pl.when(pl.program_id(0) == 0)
    def _():
        acc_out[...] = acc_ref[...]

    factor = scale_ref[...].astype(jnp.float32) * (1.0 / 127.0)
    peer_new = peer_ref[...] + coded_ref[...].astype(jnp.float32) * factor
    public_new = public_new_ref[...]
    params_new = params_ref[...] + MIX * (peer_new - public_new)
    peer_out[...] = peer_new
    params_out[...] = params_new
    distance = params_new - public_new
    square = distance * distance
    row = jnp.sum(square, axis=0, keepdims=True)
    total = row[:, :128]
    for k in range(1, row.shape[1] // 128):
        total += row[:, k * 128 : (k + 1) * 128]
    acc_out[...] += total


def combine(params, public_new, peer, coded, scale, acc, outs, piece):
    b, c0, cw = piece
    tile = min(256, cw)
    base = c0 // tile
    here = pl.BlockSpec((BLOCK, tile), lambda j: (b, base + j))
    whole = pl.BlockSpec((1, 128), lambda j: (0, 0))
    any_spec = pl.BlockSpec(memory_space=pl.ANY)
    args = [params, public_new, peer, coded, scale, acc]
    specs = [
        here,
        here,
        here,
        pl.BlockSpec((BLOCK, tile), lambda j: (0, j)),
        pl.BlockSpec((1, tile), lambda j: (0, j)),
        whole,
    ]
    aliases = {}
    if outs is not None:
        args += list(outs)
        specs += [any_spec, any_spec]
        aliases = {6: 0, 7: 1}
    full = jax.ShapeDtypeStruct(params.shape, jnp.float32)
    return pl.pallas_call(
        comb_kernel,
        grid=(cw // tile,),
        in_specs=specs,
        out_specs=[here, here, whole],
        out_shape=[full, full, jax.ShapeDtypeStruct((1, 128), jnp.float32)],
        input_output_aliases=aliases,
        cost_estimate=cost(BLOCK * cw, 14, 8),
        compiler_params=pltpu.CompilerParams(vmem_limit_bytes=8 << 20),
    )(*args)


def total_kernel(n, inverse, part_ref, out_ref, rows, send_sem, recv_sem):
    me = lax.axis_index("node")
    barrier = pltpu.get_barrier_semaphore()

    def greet(k, carry):
        pl.semaphore_signal(
            barrier, inc=1, device_id=(lax.rem(me + k, n),), device_id_type=pl.DeviceIdType.MESH
        )
        return carry

    lax.fori_loop(1, n, greet, 0)
    pl.semaphore_wait(barrier, n - 1)

    def copy(k):
        return pltpu.make_async_remote_copy(
            src_ref=part_ref,
            dst_ref=rows.at[me],
            send_sem=send_sem.at[k],
            recv_sem=recv_sem.at[me],
            device_id=(lax.rem(me + k, n),),
            device_id_type=pl.DeviceIdType.MESH,
        )

    def send(k, carry):
        copy(k).start()
        return carry

    lax.fori_loop(1, n, send, 0)
    rows[me] = part_ref[...]

    def arrive(k, carry):
        source = lax.rem(me + k, n)
        pltpu.make_async_remote_copy(
            src_ref=part_ref,
            dst_ref=rows.at[source],
            send_sem=send_sem.at[k],
            recv_sem=recv_sem.at[source],
            device_id=(source,),
            device_id_type=pl.DeviceIdType.MESH,
        ).wait()
        return carry

    lax.fori_loop(1, n, arrive, 0)
    summed = jnp.sum(rows[...], axis=0)
    out_ref[...] = jnp.broadcast_to(jnp.sum(summed, axis=1, keepdims=True) * inverse, out_ref.shape)


def total(part, n, count):
    return pl.pallas_call(
        partial(total_kernel, n, 1.0 / count),
        in_specs=[pl.BlockSpec(memory_space=pltpu.VMEM)],
        out_specs=pl.BlockSpec(memory_space=pltpu.VMEM),
        out_shape=jax.ShapeDtypeStruct((1, 128), jnp.float32),
        scratch_shapes=[
            pltpu.VMEM((n, 1, 128), jnp.float32),
            pltpu.SemaphoreType.DMA((n,)),
            pltpu.SemaphoreType.DMA((n,)),
        ],
        compiler_params=pltpu.CompilerParams(
            collective_id=0, has_side_effects=True, vmem_limit_bytes=4 << 20
        ),
    )(part)


def gossip(bit, params, public, peer_public):
    return gossip_round(bit, params, public, peer_public)


def gossip_round(bit, params, public, peer_public):
    n = lax.axis_size("node")
    pairs = [(source, source ^ (1 << bit)) for source in range(n)]
    pieces = chunk_list(*params.shape)
    public_new = None
    received = []
    for piece in pieces:
        coded, scale, public_new = encode(params, public, public_new, piece)
        got_scale = lax.ppermute(scale, "node", pairs)
        got_coded = lax.ppermute(coded, "node", pairs)
        received.append((got_coded, got_scale))
    acc = jnp.zeros((1, 128), jnp.float32)
    outs = None
    for piece, (coded, scale) in zip(pieces, received):
        params_new, peer_new, acc = combine(
            params, public_new, peer_public, coded, scale, acc, outs, piece
        )
        outs = (params_new, peer_new)
    return (*outs, public_new, acc)


def shards(params, public, peer_public, round_index):
    n = lax.axis_size("node")
    bit_count = n.bit_length() - 1
    chosen_bit = round_index[0] % bit_count
    row_count, col_count = params.shape
    branches = [partial(gossip, bit) for bit in range(bit_count)]
    params_new, peer_new, public_new, acc = lax.switch(
        chosen_bit, branches, params, public, peer_public
    )
    gap = total(acc, n, n * row_count * col_count)
    return (params_new, public_new, peer_new, gap[0, 0])


def solution(mesh):
    in_specs = (P("node", None), P("node", None), P("node", None), P())
    out_specs = (P("node", None), P("node", None), P("node", None), P())
    return jax.shard_map(shards, mesh=mesh, in_specs=in_specs, out_specs=out_specs, check_vma=False)
```

```python
from functools import partial

import jax
import jax.numpy as jnp
from jax import lax
from jax.experimental import pallas as pl
from jax.experimental.pallas import tpu as pltpu
from jax.sharding import PartitionSpec as P

BLOCK = 128
MIX = 0.4
WIDE = 512
STRIP = 128

def swap_kernel(
    bit,
    params_hbm,
    public_hbm,
    peer_hbm,
    params_out,
    public_out,
    peer_out,
    acc_out,
    params_in,
    public_in,
    peer_in,
    coded,
    scale,
    got_coded,
    got_scale,
    load_sem,
    peer_sem,
    send_sem,
    recv_sem,
):
    chunks = coded.shape[0]
    across = params_hbm.shape[1] // WIDE
    me = lax.axis_index("node")
    mask = 1 << bit
    other = me + mask - 2 * mask * (me // mask % 2)

    barrier = pltpu.get_barrier_semaphore()
    pl.semaphore_signal(
        barrier, inc=1, device_id=(other,), device_id_type=pl.DeviceIdType.MESH
    )

    def place(k):
        rows = pl.ds(pl.multiple_of(k // across * BLOCK, BLOCK), BLOCK)
        return rows, pl.multiple_of(k % across * WIDE, WIDE)

    def load(k, source, target, sem):
        rows, first = place(k)
        here = (rows, pl.ds(first, WIDE))
        return pltpu.make_async_copy(source.at[here], target.at[here], sem)

    def send(k, part):
        source, target = ((coded, got_coded), (scale, got_scale))[part]
        return pltpu.make_async_remote_copy(
            src_ref=source.at[k],
            dst_ref=target.at[k],
            send_sem=send_sem.at[part, k],
            recv_sem=recv_sem.at[part, k],
            device_id=(other,),
            device_id_type=pl.DeviceIdType.MESH,
        )

    def begin(k, carry):
        load(k, params_hbm, params_in, load_sem.at[0, k]).start()
        load(k, public_hbm, public_in, load_sem.at[1, k]).start()
        return carry

    lax.fori_loop(0, chunks, begin, 0)

    def begin_peer(k, carry):
        load(k, peer_hbm, peer_in, peer_sem.at[k]).start()
        return carry

    lax.fori_loop(0, chunks, begin_peer, 0)

    def encode(k, carry):
        rows, first = place(k)
        load(k, params_hbm, params_in, load_sem.at[0, k]).wait()
        load(k, public_hbm, public_in, load_sem.at[1, k]).wait()
        for strip in range(0, WIDE, STRIP):
            columns = pl.ds(pl.multiple_of(first + strip, STRIP), STRIP)
            difference = params_in[rows, columns] - public_in[rows, columns]
            peak = jnp.max(jnp.abs(difference), axis=0, keepdims=True) + 1e-06
            rounded = peak.astype(jnp.bfloat16)
            scale[k, :, strip : strip + STRIP] = rounded
            wide = rounded.astype(jnp.float32)
            level = jnp.floor(difference / wide * 127.0 + 0.5)
            coded[k, :, strip : strip + STRIP] = level.astype(jnp.bfloat16)
        for strip in range(0, WIDE, STRIP):
            columns = pl.ds(pl.multiple_of(first + strip, STRIP), STRIP)
            factor = scale[k, :, strip : strip + STRIP].astype(jnp.float32) * (1.0 / 127.0)
            level = coded[k, :, strip : strip + STRIP].astype(jnp.float32)
            public_out[rows, columns] = public_in[rows, columns] + level * factor

        @pl.when(k == 0)
        def _():
            pl.semaphore_wait(barrier, 1)

        send(k, 1).start()
        send(k, 0).start()
        return carry

    lax.fori_loop(0, chunks, encode, 0)

    def combine(k, total):
        rows, first = place(k)
        load(k, peer_hbm, peer_in, peer_sem.at[k]).wait()
        send(k, 1).wait_recv()
        send(k, 0).wait_recv()
        for strip in range(0, WIDE, STRIP):
            columns = pl.ds(pl.multiple_of(first + strip, STRIP), STRIP)
            factor = got_scale[k, :, strip : strip + STRIP].astype(jnp.float32) * (1.0 / 127.0)
            level = got_coded[k, :, strip : strip + STRIP].astype(jnp.float32)
            peer_new = peer_in[rows, columns] + level * factor
            public_new = public_out[rows, columns]
            params_new = params_in[rows, columns] + MIX * (peer_new - public_new)
            peer_out[rows, columns] = peer_new
            params_out[rows, columns] = params_new
            distance = params_new - public_new
            total = total + jnp.sum(distance * distance, axis=0, keepdims=True)
        return total

    acc_out[...] = lax.fori_loop(0, chunks, combine, jnp.zeros((1, STRIP), jnp.float32))

    def drain(k, carry):
        send(k, 1).wait_send()
        send(k, 0).wait_send()
        return carry

    lax.fori_loop(0, chunks, drain, 0)


def store_kernel(*refs):
    sources, targets, sem = refs[:3], refs[3:6], refs[6]
    copies = [pltpu.make_async_copy(a, b, sem.at[i]) for i, (a, b) in enumerate(zip(sources, targets))]
    for copy in copies:
        copy.start()
    for copy in copies:
        copy.wait()


def store(*arrays):
    full = jax.ShapeDtypeStruct(arrays[0].shape, arrays[0].dtype)
    return pl.pallas_call(
        store_kernel,
        in_specs=[pl.BlockSpec(memory_space=pltpu.VMEM)] * 3,
        out_specs=[pl.BlockSpec(memory_space=pl.ANY)] * 3,
        out_shape=[full] * 3,
        scratch_shapes=[pltpu.SemaphoreType.DMA((3,))],
        compiler_params=pltpu.CompilerParams(vmem_limit_bytes=1 << 20),
    )(*arrays)


def round_of(bit, params, public, peer_public):
    *results, acc = swap(bit, params, public, peer_public)
    return (*store(*results), acc)


def swap(bit, params, public, peer_public):
    row_count, col_count = params.shape
    chunks = row_count // BLOCK * (col_count // WIDE)
    full = pltpu.VMEM(params.shape, jnp.float32)
    vmem = pl.BlockSpec(memory_space=pltpu.VMEM)
    return pl.pallas_call(
        partial(swap_kernel, bit),
        in_specs=[pl.BlockSpec(memory_space=pl.ANY)] * 3,
        out_specs=[vmem] * 4,
        out_shape=[full, full, full, jax.ShapeDtypeStruct((1, STRIP), jnp.float32)],
        scratch_shapes=[
            pltpu.VMEM(params.shape, jnp.float32),
            pltpu.VMEM(params.shape, jnp.float32),
            pltpu.VMEM(params.shape, jnp.float32),
            pltpu.VMEM((chunks, BLOCK, WIDE), jnp.bfloat16),
            pltpu.VMEM((chunks, 1, WIDE), jnp.bfloat16),
            pltpu.VMEM((chunks, BLOCK, WIDE), jnp.bfloat16),
            pltpu.VMEM((chunks, 1, WIDE), jnp.bfloat16),
            pltpu.SemaphoreType.DMA((2, chunks)),
            pltpu.SemaphoreType.DMA((chunks,)),
            pltpu.SemaphoreType.DMA((2, chunks)),
            pltpu.SemaphoreType.DMA((2, chunks)),
        ],
        cost_estimate=pl.CostEstimate(
            flops=30 * row_count * col_count,
            bytes_accessed=170 * row_count * col_count,
            transcendentals=0,
        ),
        compiler_params=pltpu.CompilerParams(
            collective_id=bit + 1, has_side_effects=True, vmem_limit_bytes=40 << 20
        ),
    )(params, public, peer_public)


def total_kernel(n, inverse, part_ref, out_ref, rows, send_sem, recv_sem):
    me = lax.axis_index("node")
    barrier = pltpu.get_barrier_semaphore()

    def greet(k, carry):
        pl.semaphore_signal(
            barrier, inc=1, device_id=(lax.rem(me + k, n),), device_id_type=pl.DeviceIdType.MESH
        )
        return carry

    lax.fori_loop(1, n, greet, 0)
    pl.semaphore_wait(barrier, n - 1)

    def copy(k):
        return pltpu.make_async_remote_copy(
            src_ref=part_ref,
            dst_ref=rows.at[me],
            send_sem=send_sem.at[k],
            recv_sem=recv_sem.at[me],
            device_id=(lax.rem(me + k, n),),
            device_id_type=pl.DeviceIdType.MESH,
        )

    def send(k, carry):
        copy(k).start()
        return carry

    lax.fori_loop(1, n, send, 0)
    rows[me] = part_ref[...]

    def arrive(k, carry):
        source = lax.rem(me + k, n)
        pltpu.make_async_remote_copy(
            src_ref=part_ref,
            dst_ref=rows.at[source],
            send_sem=send_sem.at[k],
            recv_sem=recv_sem.at[source],
            device_id=(source,),
            device_id_type=pl.DeviceIdType.MESH,
        ).wait()
        return carry

    lax.fori_loop(1, n, arrive, 0)
    summed = jnp.sum(rows[...], axis=0)
    out_ref[...] = jnp.broadcast_to(jnp.sum(summed, axis=1, keepdims=True) * inverse, out_ref.shape)


def total(part, n, count):
    return pl.pallas_call(
        partial(total_kernel, n, 1.0 / count),
        in_specs=[pl.BlockSpec(memory_space=pltpu.VMEM)],
        out_specs=pl.BlockSpec(memory_space=pltpu.VMEM),
        out_shape=jax.ShapeDtypeStruct((1, 128), jnp.float32),
        scratch_shapes=[
            pltpu.VMEM((n, 1, 128), jnp.float32),
            pltpu.SemaphoreType.DMA((n,)),
            pltpu.SemaphoreType.DMA((n,)),
        ],
        compiler_params=pltpu.CompilerParams(
            collective_id=0, has_side_effects=True, vmem_limit_bytes=4 << 20
        ),
    )(part)


def shards(params, public, peer_public, round_index):
    n = lax.axis_size("node")
    bit_count = n.bit_length() - 1
    chosen_bit = round_index[0] % bit_count
    row_count, col_count = params.shape
    branches = [partial(round_of, bit) for bit in range(bit_count)]
    params_new, public_new, peer_new, acc = lax.switch(
        chosen_bit, branches, params, public, peer_public
    )
    gap = total(acc, n, n * row_count * col_count)
    return (params_new, public_new, peer_new, gap[0, 0])


def solution(mesh):
    in_specs = (P("node", None), P("node", None), P("node", None), P())
    out_specs = (P("node", None), P("node", None), P("node", None), P())
    return jax.shard_map(shards, mesh=mesh, in_specs=in_specs, out_specs=out_specs, check_vma=False)
```

```python
from functools import partial

import jax
import jax.numpy as jnp
from jax import lax
from jax.experimental import pallas as pl
from jax.experimental.pallas import tpu as pltpu
from jax.sharding import PartitionSpec as P

BLOCK = 128
MIX = 0.4
WIDE = 512
STRIP = 128

def swap_kernel(
    bit,
    inverse,
    params_hbm,
    public_hbm,
    peer_hbm,
    params_out,
    public_out,
    peer_out,
    gap_out,
    params_in,
    public_in,
    peer_in,
    coded,
    scale,
    got_coded,
    got_scale,
    load_sem,
    peer_sem,
    send_sem,
    recv_sem,
    part,
    rows_in,
    part_send_sem,
    part_recv_sem,
):
    chunks = coded.shape[0]
    across = params_hbm.shape[1] // WIDE
    me = lax.axis_index("node")
    mask = 1 << bit
    other = me + mask - 2 * mask * (me // mask % 2)

    barrier = pltpu.get_barrier_semaphore()
    n = rows_in.shape[0]

    def greet(k, carry):
        pl.semaphore_signal(
            barrier, inc=1, device_id=(lax.rem(me + k, n),), device_id_type=pl.DeviceIdType.MESH
        )
        return carry

    lax.fori_loop(1, n, greet, 0)

    def place(k):
        rows = pl.ds(pl.multiple_of(k // across * BLOCK, BLOCK), BLOCK)
        return rows, pl.multiple_of(k % across * WIDE, WIDE)

    def load(k, source, target, sem):
        rows, first = place(k)
        here = (rows, pl.ds(first, WIDE))
        return pltpu.make_async_copy(source.at[here], target.at[here], sem)

    def send(k, part):
        source, target = ((coded, got_coded), (scale, got_scale))[part]
        return pltpu.make_async_remote_copy(
            src_ref=source.at[k],
            dst_ref=target.at[k],
            send_sem=send_sem.at[part, k],
            recv_sem=recv_sem.at[part, k],
            device_id=(other,),
            device_id_type=pl.DeviceIdType.MESH,
        )

    def begin(k, carry):
        load(k, params_hbm, params_in, load_sem.at[0, k]).start()
        load(k, public_hbm, public_in, load_sem.at[1, k]).start()
        return carry

    lax.fori_loop(0, chunks, begin, 0)

    def begin_peer(k, carry):
        load(k, peer_hbm, peer_in, peer_sem.at[k]).start()
        return carry

    lax.fori_loop(0, chunks, begin_peer, 0)

    def encode(k, carry):
        rows, first = place(k)
        load(k, params_hbm, params_in, load_sem.at[0, k]).wait()
        load(k, public_hbm, public_in, load_sem.at[1, k]).wait()
        for strip in range(0, WIDE, STRIP):
            columns = pl.ds(pl.multiple_of(first + strip, STRIP), STRIP)
            difference = params_in[rows, columns] - public_in[rows, columns]
            peak = jnp.max(jnp.abs(difference), axis=0, keepdims=True) + 1e-06
            rounded = peak.astype(jnp.bfloat16)
            scale[k, :, strip : strip + STRIP] = rounded
            wide = rounded.astype(jnp.float32)
            level = jnp.floor(difference / wide * 127.0 + 0.5)
            coded[k, :, strip : strip + STRIP] = level.astype(jnp.bfloat16)
        for strip in range(0, WIDE, STRIP):
            columns = pl.ds(pl.multiple_of(first + strip, STRIP), STRIP)
            factor = scale[k, :, strip : strip + STRIP].astype(jnp.float32) * (1.0 / 127.0)
            level = coded[k, :, strip : strip + STRIP].astype(jnp.float32)
            public_out[rows, columns] = public_in[rows, columns] + level * factor

        @pl.when(k == 0)
        def _():
            pl.semaphore_wait(barrier, n - 1)

        send(k, 1).start()
        send(k, 0).start()
        return carry

    lax.fori_loop(0, chunks, encode, 0)

    def combine(k, total):
        rows, first = place(k)
        load(k, peer_hbm, peer_in, peer_sem.at[k]).wait()
        send(k, 1).wait_recv()
        send(k, 0).wait_recv()
        for strip in range(0, WIDE, STRIP):
            columns = pl.ds(pl.multiple_of(first + strip, STRIP), STRIP)
            factor = got_scale[k, :, strip : strip + STRIP].astype(jnp.float32) * (1.0 / 127.0)
            level = got_coded[k, :, strip : strip + STRIP].astype(jnp.float32)
            peer_new = peer_in[rows, columns] + level * factor
            public_new = public_out[rows, columns]
            params_new = params_in[rows, columns] + MIX * (peer_new - public_new)
            peer_out[rows, columns] = peer_new
            params_out[rows, columns] = params_new
            distance = params_new - public_new
            total = total + jnp.sum(distance * distance, axis=0, keepdims=True)
        return total

    part[...] = lax.fori_loop(0, chunks, combine, jnp.zeros((1, STRIP), jnp.float32))

    def drain(k, carry):
        send(k, 1).wait_send()
        send(k, 0).wait_send()
        return carry

    lax.fori_loop(0, chunks, drain, 0)

    def row_copy(k, owner, target):
        return pltpu.make_async_remote_copy(
            src_ref=part,
            dst_ref=rows_in.at[owner],
            send_sem=part_send_sem.at[k],
            recv_sem=part_recv_sem.at[owner],
            device_id=(target,),
            device_id_type=pl.DeviceIdType.MESH,
        )

    def send_row(k, carry):
        row_copy(k, me, lax.rem(me + k, n)).start()
        return carry

    lax.fori_loop(1, n, send_row, 0)
    rows_in[me] = part[...]

    def take_row(k, carry):
        source = lax.rem(me + k, n)
        row_copy(k, source, source).wait()
        return carry

    lax.fori_loop(1, n, take_row, 0)
    summed = jnp.sum(rows_in[...], axis=0)
    gap_out[...] = jnp.broadcast_to(jnp.sum(summed, axis=1, keepdims=True) * inverse, gap_out.shape)


def store_kernel(*refs):
    sources, targets, sem = refs[:3], refs[3:6], refs[6]
    copies = [pltpu.make_async_copy(a, b, sem.at[i]) for i, (a, b) in enumerate(zip(sources, targets))]
    for copy in copies:
        copy.start()
    for copy in copies:
        copy.wait()


def store(*arrays):
    full = jax.ShapeDtypeStruct(arrays[0].shape, arrays[0].dtype)
    return pl.pallas_call(
        store_kernel,
        in_specs=[pl.BlockSpec(memory_space=pltpu.VMEM)] * 3,
        out_specs=[pl.BlockSpec(memory_space=pl.ANY)] * 3,
        out_shape=[full] * 3,
        scratch_shapes=[pltpu.SemaphoreType.DMA((3,))],
        compiler_params=pltpu.CompilerParams(vmem_limit_bytes=1 << 20),
    )(*arrays)


def round_of(bit, params, public, peer_public):
    *results, acc = swap(bit, params, public, peer_public)
    return (*store(*results), acc)


def swap(bit, params, public, peer_public):
    row_count, col_count = params.shape
    chunks = row_count // BLOCK * (col_count // WIDE)
    n = lax.axis_size("node")
    inverse = 1.0 / (n * row_count * col_count)
    full = pltpu.VMEM(params.shape, jnp.float32)
    vmem = pl.BlockSpec(memory_space=pltpu.VMEM)
    return pl.pallas_call(
        partial(swap_kernel, bit, inverse),
        in_specs=[pl.BlockSpec(memory_space=pl.ANY)] * 3,
        out_specs=[vmem] * 4,
        out_shape=[full, full, full, jax.ShapeDtypeStruct((1, STRIP), jnp.float32)],
        scratch_shapes=[
            pltpu.VMEM(params.shape, jnp.float32),
            pltpu.VMEM(params.shape, jnp.float32),
            pltpu.VMEM(params.shape, jnp.float32),
            pltpu.VMEM((chunks, BLOCK, WIDE), jnp.bfloat16),
            pltpu.VMEM((chunks, 1, WIDE), jnp.bfloat16),
            pltpu.VMEM((chunks, BLOCK, WIDE), jnp.bfloat16),
            pltpu.VMEM((chunks, 1, WIDE), jnp.bfloat16),
            pltpu.SemaphoreType.DMA((2, chunks)),
            pltpu.SemaphoreType.DMA((chunks,)),
            pltpu.SemaphoreType.DMA((2, chunks)),
            pltpu.SemaphoreType.DMA((2, chunks)),
            pltpu.VMEM((1, STRIP), jnp.float32),
            pltpu.VMEM((n, 1, STRIP), jnp.float32),
            pltpu.SemaphoreType.DMA((n,)),
            pltpu.SemaphoreType.DMA((n,)),
        ],
        cost_estimate=pl.CostEstimate(
            flops=30 * row_count * col_count,
            bytes_accessed=170 * row_count * col_count,
            transcendentals=0,
        ),
        compiler_params=pltpu.CompilerParams(
            collective_id=bit + 1, has_side_effects=True, vmem_limit_bytes=40 << 20
        ),
    )(params, public, peer_public)


def shards(params, public, peer_public, round_index):
    n = lax.axis_size("node")
    bit_count = n.bit_length() - 1
    chosen_bit = round_index[0] % bit_count
    branches = [partial(round_of, bit) for bit in range(bit_count)]
    params_new, public_new, peer_new, gap = lax.switch(
        chosen_bit, branches, params, public, peer_public
    )
    return (params_new, public_new, peer_new, gap[0, 0])


def solution(mesh):
    in_specs = (P("node", None), P("node", None), P("node", None), P())
    out_specs = (P("node", None), P("node", None), P("node", None), P())
    return jax.shard_map(shards, mesh=mesh, in_specs=in_specs, out_specs=out_specs, check_vma=False)
```
